32 devices in a mesh: gx: 16 (over z, y, x), gy: 2 (over core).
Axes of the slice: x: 2, y: 2, z: 4, core: 2. Of those that a mesh axis runs over, the one named last changes fastest.
Arguments:
- sources: bfloat16 [2048, 8, 128], P(('gx', 'gy')), may hold values from -6 to 6
- owners: int32 [2048, 1], P(('gx', 'gy')), may hold values from 0 to 15; in each aligned block of 64 rows (0 to 63, 64 to 127, ...) at most 8 rows name the same one
- strip_rows: int32 [2048], P(('gx', 'gy')), may hold values from 0 to 255
- panel_counts: int32 [2048], P(('gx', 'gy')), may hold values from 1 to 128
- arrival_bins: int32 [4096, 4, 128], P('gx'), may hold values from 0 to 254
- arrival_fracs: float32 [4096, 4, 128], P('gx'), may hold values from 0 to 1
- gain_table: bfloat16 [4096, 8, 4, 1024], P('gx'), may hold values from -0.125 to 0.125
Outputs:
- signals: float32 [1024, 4, 256], P(('gx', 'gy'))
The draws below stay inside these ranges and needn't reach their ends.
Inputs may be any that keep to these rules, and one draw needn't show every extreme that they name: `owners`: among the rows of one device, at most 8 strips name one patch, a bound that some block reaches.
All inputs are finite; a program needn't handle non-finite values.
Results may differ from the reference program's by a relative error of at most 0.0044.
Values may be sent and summed in bfloat16 or wider, within the bound.
A program may use at most 768 MiB of HBM per device.

```python
import math
import jax
import jax.numpy as jnp
import numpy as np
from jax import lax

TERMS = 8
SP = 128
NBIN = 256
NOB = 4
OBS_BLOCK = 1024
STRIP_DEV = 64
ROWS = 256
CAP = 8
STRIPS = 2048
TROWS = 4096
N_GX = 16


def set_ends(array, stream_key, low, high):
    longest = array.shape.index(max(array.shape))
    spots = []
    for shift in (0, 1):
        where = [jax.random.randint(jax.random.fold_in(stream_key, axis), (), 0, length) for axis, length in enumerate(array.shape)]
        where[longest] = (where[longest] + shift) % array.shape[longest]
        spots.append(tuple(where))
    return array.at[spots[0]].set(low).at[spots[1]].set(high)


def spiked(drawn, key, source, target, shards_of, factor):
    owner, partner = [(jnp.arange(drawn.shape[axis_at]) // (drawn.shape[axis_at] // shards_of)).reshape([-1 if axis == axis_at else 1 for axis in range(drawn.ndim)]) for axis_at in (source, target)]
    chosen = jax.random.permutation(key, shards_of)[partner]
    strong = (owner == chosen) | (owner == (partner + shards_of // 2) % shards_of)
    return jnp.where(strong, factor * drawn, drawn)


def level_of(own_key, shape, pieces, low, largest):
    def one(position, parts):
        heights = jax.random.uniform(jax.random.fold_in(jax.random.fold_in(own_key, 6), position), (parts,), jnp.float32, low / len(pieces), largest / len(pieces))
        return jnp.repeat(jnp.exp(heights), shape[position] // parts).reshape((-1,) + (1,) * (len(shape) - position - 1))

    level = one(*pieces[0])
    for cut in pieces[1:]:
        level = level * one(*cut)
    return level


def assign_block(key, own, number, rows, count, top, most, slope):
    order = jax.random.permutation(key, count)
    crowded, usual = portions_of(count, rows * top, most, slope, True), portions_of(count, rows * top, most, slope, False)
    places = jnp.arange(count)

    def named(sizes, turn):
        used = int((sizes > 0).sum())
        fixed = max(1, used // 4)
        passed = fixed + (places - fixed + turn * (used - fixed)) % max(1, count - fixed)
        return jnp.zeros((count,), jnp.int32).at[order[jnp.where(places < fixed, places, passed)]].set(jnp.asarray(sizes, jnp.int32))

    sizes = jnp.where(number % 4 == 0, named(crowded, number // 4), named(usual, number - number // 4 - 1))
    mixed = jax.random.permutation(jax.random.fold_in(own, 3), count)
    donor, receiver = mixed[0:count // 2 * 2:2], mixed[1:count // 2 * 2:2]
    slack = jnp.minimum(sizes[donor] - 1, most - sizes[receiver]) // 2
    slack = jnp.where((donor == order[0]) | (receiver == order[0]) | (sizes[receiver] == 0), 0, jnp.maximum(slack, 0))
    passed = jax.random.randint(jax.random.fold_in(own, 4), (count // 2,), 0, 1 << 20) % (slack + 1)
    sizes = sizes.at[donor].add(-passed).at[receiver].add(passed)
    members = jnp.searchsorted(jnp.cumsum(sizes), jnp.arange(rows * top), side="right").astype(jnp.int32)
    listing = members.reshape(top, rows).T
    listing = listing[jax.random.permutation(jax.random.fold_in(own, 1), rows)]
    turn = jax.random.randint(jax.random.fold_in(own, 2), (rows, 1), 0, top)
    return jnp.take_along_axis(listing, (jnp.arange(top)[None, :] + turn) % top, axis=1)


def portions_of(count, total, reach, slope, full):
    loads = [(1 << 20) // math.isqrt(standing ** slope) + 1 for standing in range(1, count + 1)]
    largest = reach if full else min(reach, max(-(-total // count), total * loads[0] // sum(loads)))
    least = 1 if total - largest >= count - 1 else 0
    holding, surplus = [largest] + [least] * (count - 1), total - largest - least * (count - 1)
    while surplus > 0:
        free = [i for i in range(1, count) if holding[i] < largest] or [i for i in range(1, count) if holding[i] < reach]
        pool, budget = sum([loads[i] for i in free]), surplus
        for i in free:
            more = min(reach - holding[i], max(1, budget * loads[i] // pool), surplus)
            holding[i] = holding[i] + more
            surplus = surplus - more
    return np.array(holding)


def gaussian(rng, dims, spread, most, shards=(), held_as=jnp.bfloat16):
    values = spread * jax.random.normal(rng, dims, jnp.float32)
    if shards:
        values = values * level_of(rng, dims, shards, -0.22, 0.18)
    return jnp.clip(values, -most, most).astype(held_as)


def bell_draw_with(key, shape, width, limit, split, heavy, kind=jnp.bfloat16):
    result = width * jax.random.normal(key, shape, jnp.float32)
    if split:
        result = result * level_of(key, shape, split, -0.22, 0.18)
    return jnp.clip(spiked(result, jax.random.fold_in(key, 3), *heavy), -limit, limit).astype(kind)


def setup_inputs(seed: int = 0) -> dict:
    arg_keys = jax.random.split(jax.random.key(seed), 8)
    sources = gaussian(arg_keys[0], (STRIPS, TERMS, SP), 1.0, 6.0, ((0, 32),))
    owners_keys = jax.random.split(jax.random.fold_in(arg_keys[1], 1), STRIPS // STRIP_DEV)
    owners_turns = jax.random.permutation(jax.random.fold_in(arg_keys[1], 3), STRIPS // STRIP_DEV)
    owners = jax.vmap(lambda own, number: assign_block(jax.random.fold_in(arg_keys[1], 2), own, number, STRIP_DEV, N_GX, 1, CAP, 2))(owners_keys, owners_turns).reshape((STRIPS, 1))
    strip_rows = set_ends(jax.random.randint(arg_keys[2], (STRIPS,), 0, ROWS), jax.random.fold_in(arg_keys[2], 1), 0, ROWS - 1).astype(jnp.int32)
    panel_counts = set_ends(jax.random.randint(arg_keys[3], (STRIPS,), 1, SP + 1), jax.random.fold_in(arg_keys[3], 1), 1, SP).astype(jnp.int32)
    arrival_bins = set_ends(jax.random.randint(arg_keys[4], (TROWS, NOB, SP), 0, NBIN - 1), jax.random.fold_in(arg_keys[4], 1), 0, (NBIN - 1) - 1).astype(jnp.int32)
    arrival_fracs = jnp.clip(1.0 * jax.random.uniform(arg_keys[5], (TROWS, NOB, SP), jnp.float32) ** level_of(arg_keys[5], (TROWS, NOB, SP), ((0, 16),), -0.2, 0.2), 0.0, 1.0)
    gain_table = bell_draw_with(arg_keys[6], (TROWS, TERMS, NOB, OBS_BLOCK), TROWS ** -0.5, 0.125, ((0, 16),), (0, 3, 16, 2.0))
    return {"sources": sources, "owners": owners, "strip_rows": strip_rows, "panel_counts": panel_counts, "arrival_bins": arrival_bins, "arrival_fracs": arrival_fracs, "gain_table": gain_table}


def interp_weights(bin_ids, fractions):
    positions = jnp.arange(NBIN, dtype=jnp.int32)
    lower = jnp.where(positions[None, None, :] == bin_ids[:, :, None], 1.0 - fractions[:, :, None], 0.0)
    upper = jnp.where(positions[None, None, :] == bin_ids[:, :, None] + 1, fractions[:, :, None], 0.0)
    return (lower + upper).astype(jnp.bfloat16)


def reference(sources, owners, strip_rows, panel_counts, arrival_bins, arrival_fracs, gain_table):
    live_mask = (jnp.arange(SP, dtype=jnp.int32)[None, :] < panel_counts[:, None]).astype(jnp.float32)
    masked = sources.astype(jnp.float32) * live_mask[:, None, :]
    global_rows = (owners[:, 0] * ROWS + strip_rows).astype(jnp.int32)
    row_sources = jax.ops.segment_sum(masked, global_rows, num_segments=ROWS * N_GX)
    row_rounded = row_sources.astype(jnp.bfloat16)

    def patch_term(running, patch_index):
        first_row = (patch_index * ROWS).astype(jnp.int32)
        patch_sources = lax.dynamic_slice_in_dim(row_rounded, first_row, ROWS, 0).astype(jnp.float32)
        patch_bins = lax.dynamic_slice_in_dim(arrival_bins, first_row, ROWS, 0)
        patch_fracs = lax.dynamic_slice_in_dim(arrival_fracs, first_row, ROWS, 0)
        patch_gains = lax.dynamic_slice_in_dim(gain_table, first_row, ROWS, 0).astype(jnp.float32)
        for block_index in range(NOB):
            weights = interp_weights(patch_bins[:, block_index, :], patch_fracs[:, block_index, :]).astype(jnp.float32)
            arrived = jnp.einsum('rkp,rpb->rkb', patch_sources, weights, precision=lax.Precision.HIGHEST)
            arrived_rounded = arrived.astype(jnp.bfloat16).astype(jnp.float32)
            added = jnp.einsum('rkt,rkb->tb', patch_gains[:, :, block_index, :], arrived_rounded, precision=lax.Precision.HIGHEST)
            running = running.at[:, block_index, :].add(added)
        return running, None

    start_value = jnp.zeros((OBS_BLOCK, NOB, NBIN), jnp.float32)
    signals, unused = lax.scan(patch_term, start_value, jnp.arange(N_GX, dtype=jnp.int32))
    return signals
```

```python
import functools

import jax
import jax.numpy as jnp
from jax import lax
from jax.experimental import pallas as pl
from jax.experimental.pallas import tpu as pltpu
from jax.sharding import PartitionSpec as P

NBIN = 256


def bin_kernel(block_ref, src_ref, bins_ref, fracs_ref, out_ref):
    block = block_ref[0]
    pairs = src_ref.shape[0] // 16
    panels = src_ref.shape[1]
    low = lax.broadcasted_iota(jnp.int32, (16, panels), 0) < 8
    spots = lax.broadcasted_iota(jnp.int32, (NBIN, panels), 0).astype(jnp.float32).astype(jnp.bfloat16)

    def weights_of(row):
        bins = bins_ref[row, pl.ds(block, 1), :].astype(jnp.float32)
        fracs = fracs_ref[row, pl.ds(block, 1), :]

        def spread(v):
            return jnp.broadcast_to(v, (NBIN, panels)).astype(jnp.bfloat16)

        first, second = spread(bins), spread(bins + 1.0)
        return jnp.where(
            spots == first,
            spread(1.0 - fracs),
            jnp.where(spots == second, spread(fracs), jnp.zeros((), jnp.bfloat16)),
        )

    def step(i, carry):
        both = src_ref[pl.ds(pl.multiple_of(i * 16, 16), 16), :].astype(jnp.float32)
        top = jnp.where(low, both, 0.0).astype(jnp.bfloat16)
        bottom = jnp.where(low, 0.0, both).astype(jnp.bfloat16)
        lhs = jnp.concatenate([top, bottom], axis=1)
        weights = jnp.concatenate([weights_of(2 * i), weights_of(2 * i + 1)], axis=1)
        got = lax.dot_general(
            lhs, weights, (((1,), (1,)), ((), ())), preferred_element_type=jnp.float32
        )
        out_ref[pl.ds(pl.multiple_of(i * 16, 16), 16), :] = got.astype(jnp.bfloat16)
        return carry

    lax.fori_loop(0, pairs, step, 0, unroll=4)


def bin_rows(block, src, bins, fracs):
    rows = src.shape[0]
    return pl.pallas_call(
        bin_kernel,
        out_shape=jax.ShapeDtypeStruct((rows, NBIN), jnp.bfloat16),
        in_specs=[
            pl.BlockSpec(memory_space=pltpu.SMEM),
            pl.BlockSpec(memory_space=pltpu.VMEM),
            pl.BlockSpec(memory_space=pltpu.VMEM),
            pl.BlockSpec(memory_space=pltpu.VMEM),
        ],
        out_specs=pl.BlockSpec(memory_space=pltpu.VMEM),
        name="bin_rows",
        cost_estimate=pl.CostEstimate(flops=rows * 2 * 256 * 256, bytes_accessed=rows * 1000, transcendentals=0),
    )(block, src, bins, fracs)


def on_device(sources, owners, strip_rows, panel_counts, arrival_bins, arrival_fracs, gain_table):
    strip_count, terms, panels = sources.shape
    shards = lax.axis_size("gx")
    columns = lax.axis_size("gy")
    capacity = 2 * strip_count // shards
    blocks = arrival_bins.shape[1]
    observers = gain_table.shape[3]
    rows_here = arrival_bins.shape[0]
    live_mask = (jnp.arange(panels, dtype=jnp.int32)[None, :] < panel_counts[:, None]).astype(
        jnp.bfloat16
    )
    masked = (sources * live_mask[:, None, :]).reshape(strip_count, terms * panels)
    lane = jnp.arange(128, dtype=jnp.int32)[None, :]
    coded = jnp.where(
        lane == 0,
        (strip_rows // 128)[:, None],
        jnp.where(lane == 1, (strip_rows % 128)[:, None], jnp.where(lane == 2, 1, 0)),
    ).astype(jnp.bfloat16)
    payload = jnp.concatenate([masked, coded], axis=1)
    targets = owners[:, 0]
    earlier = (
        jnp.arange(strip_count, dtype=jnp.int32)[None, :]
        < jnp.arange(strip_count, dtype=jnp.int32)[:, None]
    )
    order_in = jnp.sum(
        jnp.where(earlier & (targets[None, :] == targets[:, None]), 1, 0).astype(jnp.int32), axis=1
    )
    slot_of = targets * capacity + order_in
    placing = jnp.arange(shards * capacity, dtype=jnp.int32)[:, None] == slot_of[None, :]
    send = jnp.dot(
        placing.astype(jnp.bfloat16), payload, preferred_element_type=jnp.float32
    ).astype(jnp.bfloat16)
    got = lax.all_to_all(send, "gx", split_axis=0, concat_axis=0, tiled=True)
    got = lax.all_gather(got, "gy", axis=0, tiled=True)
    codes = got[:, terms * panels :].astype(jnp.int32)
    got_rows = jnp.where(codes[:, 2] > 0, codes[:, 0] * 128 + codes[:, 1], -1)
    row_hot = (jnp.arange(rows_here, dtype=jnp.int32)[:, None] == got_rows[None, :]).astype(
        jnp.bfloat16
    )
    row_sources = jnp.dot(
        row_hot, got[:, : terms * panels], preferred_element_type=jnp.float32
    ).astype(jnp.bfloat16)
    src = row_sources.reshape(rows_here * terms, panels)
    per = blocks // columns
    first = lax.axis_index("gy") * per
    gains = lax.dynamic_slice_in_dim(gain_table, first, per, 2)
    sums = []
    share = observers // (shards * columns)
    for o in range(per):
        block = (first + o).astype(jnp.int32).reshape(1)
        arrived = bin_rows(block, src, arrival_bins, arrival_fracs)
        partial = jnp.einsum(
            "ct,cb->tb",
            gains[:, :, o, :].reshape(rows_here * terms, observers),
            arrived,
            preferred_element_type=jnp.float32,
        ).astype(jnp.bfloat16)
        parts = lax.all_to_all(partial, ("gx", "gy"), split_axis=0, concat_axis=0, tiled=True)
        sums.append(
            jnp.sum(parts.reshape(shards, columns, share, NBIN).astype(jnp.float32), axis=0)
        )
    return jnp.stack(sums, axis=1).transpose(2, 0, 1, 3).reshape(share, blocks, NBIN)


def solution(mesh):
    placed = (
        P(("gx", "gy"), None, None),
        P(("gx", "gy"), None),
        P(("gx", "gy")),
        P(("gx", "gy")),
        P("gx", None, None),
        P("gx", None, None),
        P("gx", None, None, None),
    )
    return jax.shard_map(
        on_device,
        mesh=mesh,
        in_specs=placed,
        out_specs=P(("gx", "gy"), None, None),
        check_vma=False,
    )
```

```python
import functools

import jax
import jax.numpy as jnp
from jax import lax
from jax.experimental import pallas as pl
from jax.experimental.pallas import tpu as pltpu
from jax.sharding import PartitionSpec as P

NBIN = 256


def bin_kernel(block_ref, src_ref, bins_ref, fracs_ref, out_ref):
    block = block_ref[0]
    pairs = src_ref.shape[0] // 16
    panels = src_ref.shape[1]
    low = lax.broadcasted_iota(jnp.int32, (16, panels), 0) < 8
    spots = lax.broadcasted_iota(jnp.int32, (NBIN, panels), 0).astype(jnp.float32).astype(jnp.bfloat16)

    def weights_of(row):
        bins = bins_ref[row, pl.ds(block, 1), :].astype(jnp.float32)
        fracs = fracs_ref[row, pl.ds(block, 1), :]

        def spread(v):
            return jnp.broadcast_to(v, (NBIN, panels)).astype(jnp.bfloat16)

        first, second = spread(bins), spread(bins + 1.0)
        return jnp.where(
            spots == first,
            spread(1.0 - fracs),
            jnp.where(spots == second, spread(fracs), jnp.zeros((), jnp.bfloat16)),
        )

    def step(i, carry):
        both = src_ref[pl.ds(pl.multiple_of(i * 16, 16), 16), :].astype(jnp.float32)
        top = jnp.where(low, both, 0.0).astype(jnp.bfloat16)
        bottom = jnp.where(low, 0.0, both).astype(jnp.bfloat16)
        lhs = jnp.concatenate([top, bottom], axis=1)
        weights = jnp.concatenate([weights_of(2 * i), weights_of(2 * i + 1)], axis=1)
        got = lax.dot_general(
            lhs, weights, (((1,), (1,)), ((), ())), preferred_element_type=jnp.float32
        )
        out_ref[pl.ds(pl.multiple_of(i * 16, 16), 16), :] = got.astype(jnp.bfloat16)
        return carry

    lax.fori_loop(0, pairs, step, 0, unroll=4)


def bin_rows(block, src, bins, fracs):
    rows = src.shape[0]
    return pl.pallas_call(
        bin_kernel,
        out_shape=jax.ShapeDtypeStruct((rows, NBIN), jnp.bfloat16),
        in_specs=[
            pl.BlockSpec(memory_space=pltpu.SMEM),
            pl.BlockSpec(memory_space=pltpu.VMEM),
            pl.BlockSpec(memory_space=pltpu.VMEM),
            pl.BlockSpec(memory_space=pltpu.VMEM),
        ],
        out_specs=pl.BlockSpec(memory_space=pltpu.VMEM),
        name="bin_rows",
        cost_estimate=pl.CostEstimate(flops=rows * 2 * 256 * 256, bytes_accessed=rows * 1000, transcendentals=0),
    )(block, src, bins, fracs)


def gained(block, gain_table, arrived):
    gains = gain_table[:, :, block, :].reshape(arrived.shape[0], gain_table.shape[3])
    return jnp.einsum("ct,cb->tb", gains, arrived, preferred_element_type=jnp.float32).astype(
        jnp.bfloat16
    )


def on_device(sources, owners, strip_rows, panel_counts, arrival_bins, arrival_fracs, gain_table):
    strip_count, terms, panels = sources.shape
    shards = lax.axis_size("gx")
    columns = lax.axis_size("gy")
    capacity = 2 * strip_count // shards
    blocks = arrival_bins.shape[1]
    observers = gain_table.shape[3]
    rows_here = arrival_bins.shape[0]
    live_mask = (jnp.arange(panels, dtype=jnp.int32)[None, :] < panel_counts[:, None]).astype(
        jnp.bfloat16
    )
    masked = (sources * live_mask[:, None, :]).reshape(strip_count, terms * panels)
    lane = jnp.arange(128, dtype=jnp.int32)[None, :]
    coded = jnp.where(
        lane == 0,
        (strip_rows // 128)[:, None],
        jnp.where(lane == 1, (strip_rows % 128)[:, None], jnp.where(lane == 2, 1, 0)),
    ).astype(jnp.bfloat16)
    payload = jnp.concatenate([masked, coded], axis=1)
    targets = owners[:, 0]
    earlier = (
        jnp.arange(strip_count, dtype=jnp.int32)[None, :]
        < jnp.arange(strip_count, dtype=jnp.int32)[:, None]
    )
    order_in = jnp.sum(
        jnp.where(earlier & (targets[None, :] == targets[:, None]), 1, 0).astype(jnp.int32), axis=1
    )
    slot_of = targets * capacity + order_in
    placing = jnp.arange(shards * capacity, dtype=jnp.int32)[:, None] == slot_of[None, :]
    send = jnp.dot(
        placing.astype(jnp.bfloat16), payload, preferred_element_type=jnp.float32
    ).astype(jnp.bfloat16)
    got = lax.all_to_all(send, "gx", split_axis=0, concat_axis=0, tiled=True)
    got = lax.all_gather(got, "gy", axis=0, tiled=True)
    codes = got[:, terms * panels :].astype(jnp.int32)
    got_rows = jnp.where(codes[:, 2] > 0, codes[:, 0] * 128 + codes[:, 1], -1)
    row_hot = (jnp.arange(rows_here, dtype=jnp.int32)[:, None] == got_rows[None, :]).astype(
        jnp.bfloat16
    )
    row_sources = jnp.dot(
        row_hot, got[:, : terms * panels], preferred_element_type=jnp.float32
    ).astype(jnp.bfloat16)
    src = row_sources.reshape(rows_here * terms, panels)
    per = blocks // columns
    first = lax.axis_index("gy") * per
    sums = []
    share = observers // (shards * columns)
    for o in range(per):
        block = (first + o).astype(jnp.int32).reshape(1)
        arrived = bin_rows(block, src, arrival_bins, arrival_fracs)
        partial = lax.switch(
            lax.axis_index("gy"),
            [functools.partial(gained, column * per + o) for column in range(columns)],
            gain_table,
            arrived,
        )
        parts = lax.all_to_all(partial, ("gx", "gy"), split_axis=0, concat_axis=0, tiled=True)
        sums.append(
            jnp.sum(parts.reshape(shards, columns, share, NBIN).astype(jnp.float32), axis=0)
        )
    return jnp.stack(sums, axis=1).transpose(2, 0, 1, 3).reshape(share, blocks, NBIN)


def solution(mesh):
    placed = (
        P(("gx", "gy"), None, None),
        P(("gx", "gy"), None),
        P(("gx", "gy")),
        P(("gx", "gy")),
        P("gx", None, None),
        P("gx", None, None),
        P("gx", None, None, None),
    )
    return jax.shard_map(
        on_device,
        mesh=mesh,
        in_specs=placed,
        out_specs=P(("gx", "gy"), None, None),
        check_vma=False,
    )
```

```python
import functools

import jax
import jax.numpy as jnp
from jax import lax
from jax.experimental import pallas as pl
from jax.experimental.pallas import tpu as pltpu
from jax.sharding import PartitionSpec as P

NBIN = 256


def bin_kernel(block_ref, src_ref, bins_ref, fracs_ref, out_ref):
    block = block_ref[0]
    pairs = src_ref.shape[0] // 16
    panels = src_ref.shape[1]
    low = lax.broadcasted_iota(jnp.int32, (16, panels), 0) < 8
    spots = lax.broadcasted_iota(jnp.int32, (NBIN, panels), 0).astype(jnp.float32).astype(jnp.bfloat16)

    def weights_of(row):
        bins = bins_ref[row, pl.ds(block, 1), :].astype(jnp.float32)
        fracs = fracs_ref[row, pl.ds(block, 1), :]

        def spread(v):
            return jnp.broadcast_to(v, (NBIN, panels)).astype(jnp.bfloat16)

        first, second = spread(bins), spread(bins + 1.0)
        return jnp.where(
            spots == first,
            spread(1.0 - fracs),
            jnp.where(spots == second, spread(fracs), jnp.zeros((), jnp.bfloat16)),
        )

    def step(i, carry):
        both = src_ref[pl.ds(pl.multiple_of(i * 16, 16), 16), :].astype(jnp.float32)
        top = jnp.where(low, both, 0.0).astype(jnp.bfloat16)
        bottom = jnp.where(low, 0.0, both).astype(jnp.bfloat16)
        lhs = jnp.concatenate([top, bottom], axis=1)
        weights = jnp.concatenate([weights_of(2 * i), weights_of(2 * i + 1)], axis=1)
        got = lax.dot_general(
            lhs, weights, (((1,), (1,)), ((), ())), preferred_element_type=jnp.float32
        )
        out_ref[pl.ds(pl.multiple_of(i * 16, 16), 16), :] = got.astype(jnp.bfloat16)
        return carry

    lax.fori_loop(0, pairs, step, 0, unroll=4)


def bin_rows(block, src, bins, fracs):
    rows = src.shape[0]
    return pl.pallas_call(
        bin_kernel,
        out_shape=jax.ShapeDtypeStruct((rows, NBIN), jnp.bfloat16),
        in_specs=[
            pl.BlockSpec(memory_space=pltpu.SMEM),
            pl.BlockSpec(memory_space=pltpu.VMEM),
            pl.BlockSpec(memory_space=pltpu.VMEM),
            pl.BlockSpec(memory_space=pltpu.VMEM),
        ],
        out_specs=pl.BlockSpec(memory_space=pltpu.VMEM),
        name="bin_rows",
        cost_estimate=pl.CostEstimate(flops=rows * 2 * 256 * 256, bytes_accessed=rows * 1000, transcendentals=0),
    )(block, src, bins, fracs)


def on_device(sources, owners, strip_rows, panel_counts, arrival_bins, arrival_fracs, gain_table):
    strip_count, terms, panels = sources.shape
    shards = lax.axis_size("gx")
    columns = lax.axis_size("gy")
    capacity = 2 * strip_count // shards
    blocks = arrival_bins.shape[1]
    observers = gain_table.shape[3]
    rows_here = arrival_bins.shape[0]
    live_mask = (jnp.arange(panels, dtype=jnp.int32)[None, :] < panel_counts[:, None]).astype(
        jnp.bfloat16
    )
    masked = (sources * live_mask[:, None, :]).reshape(strip_count, terms * panels)
    lane = jnp.arange(128, dtype=jnp.int32)[None, :]
    coded = jnp.where(
        lane == 0,
        (strip_rows // 128)[:, None],
        jnp.where(lane == 1, (strip_rows % 128)[:, None], jnp.where(lane == 2, 1, 0)),
    ).astype(jnp.bfloat16)
    payload = jnp.concatenate([masked, coded], axis=1)
    targets = owners[:, 0]
    earlier = (
        jnp.arange(strip_count, dtype=jnp.int32)[None, :]
        < jnp.arange(strip_count, dtype=jnp.int32)[:, None]
    )
    order_in = jnp.sum(
        jnp.where(earlier & (targets[None, :] == targets[:, None]), 1, 0).astype(jnp.int32), axis=1
    )
    slot_of = targets * capacity + order_in
    placing = jnp.arange(shards * capacity, dtype=jnp.int32)[:, None] == slot_of[None, :]
    send = jnp.dot(
        placing.astype(jnp.bfloat16), payload, preferred_element_type=jnp.float32
    ).astype(jnp.bfloat16)
    got = lax.all_to_all(send, "gx", split_axis=0, concat_axis=0, tiled=True)
    got = lax.all_gather(got, "gy", axis=0, tiled=True)
    codes = got[:, terms * panels :].astype(jnp.int32)
    got_rows = jnp.where(codes[:, 2] > 0, codes[:, 0] * 128 + codes[:, 1], -1)
    row_hot = (jnp.arange(rows_here, dtype=jnp.int32)[:, None] == got_rows[None, :]).astype(
        jnp.bfloat16
    )
    row_sources = jnp.dot(
        row_hot, got[:, : terms * panels], preferred_element_type=jnp.float32
    ).astype(jnp.bfloat16)
    src = row_sources.reshape(rows_here * terms, panels)
    per = blocks // columns
    first = lax.axis_index("gy") * per
    gains = lax.optimization_barrier(
        gain_table.transpose(2, 0, 1, 3).reshape(blocks, rows_here * terms, observers)
    )
    sums = []
    share = observers // (shards * columns)
    for o in range(per):
        block = (first + o).astype(jnp.int32).reshape(1)
        arrived = bin_rows(block, src, arrival_bins, arrival_fracs)
        partial = jnp.einsum(
            "ct,cb->tb",
            lax.dynamic_index_in_dim(gains, first + o, 0, keepdims=False),
            arrived,
            preferred_element_type=jnp.float32,
        ).astype(jnp.bfloat16)
        parts = lax.all_to_all(partial, ("gx", "gy"), split_axis=0, concat_axis=0, tiled=True)
        sums.append(
            jnp.sum(parts.reshape(shards, columns, share, NBIN).astype(jnp.float32), axis=0)
        )
    return jnp.stack(sums, axis=1).transpose(2, 0, 1, 3).reshape(share, blocks, NBIN)


def solution(mesh):
    placed = (
        P(("gx", "gy"), None, None),
        P(("gx", "gy"), None),
        P(("gx", "gy")),
        P(("gx", "gy")),
        P("gx", None, None),
        P("gx", None, None),
        P("gx", None, None, None),
    )
    return jax.shard_map(
        on_device,
        mesh=mesh,
        in_specs=placed,
        out_specs=P(("gx", "gy"), None, None),
        check_vma=False,
    )
```
